32 devices in a mesh: band: 4 (over y, x), grid: 8 (over z, core).
Axes of the slice: x: 2, y: 2, z: 4, core: 2. Of those that a mesh axis runs over, the one named last changes fastest.
Arguments:
- coefficients: bfloat16 [256, 18, 2048], P('grid', None, 'band'), may hold values from -0.125 to 0.125
- occupation: int32 [2048], P('band'), may hold values from 0 to 8
- shapes: bfloat16 [171, 32768], replicated, may hold values from -1.5 to 1.5
- corners: int32 [3, 256], replicated, may hold values from 0 to 256, as said below
Outputs:
- density: float32 [256, 288, 288], P('grid')
The draws below stay inside these ranges and needn't reach their ends.
Inputs may be any that keep to these rules, and one draw needn't show every extreme that they name: Every box lies inside the grid. Counting atoms by the slab floor(corners[0, a] / 32), no slab holds more than 64 atoms, some slab holds exactly 64, and every slab holds at least 16.
All inputs are finite; a program needn't handle non-finite values.
Results may differ from the reference program's by a relative error of at most 0.0029.
Values may be sent and summed in bfloat16 or wider, within the bound.
A program may use at most 192 MiB of HBM per device.

```python
import jax
import jax.numpy as jnp
import numpy as np
from jax import lax

NPROJ = 18
BOX = 32
ZS = 32
NY = 288
NX = 288
AT_DEV = 32
NPAIR = 171
ATOMS = 256
BANDS = 2048
NZ = 256
N_GRID = 8


def draw_corners(key, part):
    key_order = jax.random.fold_in(key, 11)
    key_depth = jax.random.fold_in(key, 12)
    key_row = jax.random.fold_in(key, 13)
    key_column = jax.random.fold_in(key, 14)
    key_atoms = jax.random.fold_in(key, 15)
    slab_order = jax.random.permutation(key_order, N_GRID)
    quarter = N_GRID // 4
    ranks = jnp.arange(N_GRID, dtype=jnp.int32)
    loads = jnp.where(ranks < quarter, 2 * AT_DEV, jnp.where(ranks < 2 * quarter, AT_DEV, AT_DEV // 2)).astype(jnp.int32)
    bounds = jnp.cumsum(loads).astype(jnp.int32)
    positions = jnp.arange(ATOMS, dtype=jnp.int32)
    atom_rank = jnp.sum((positions[:, None] >= bounds[None, :]).astype(jnp.int32), axis=1)
    slab = slab_order[atom_rank].astype(jnp.int32)
    top = jnp.where(slab == N_GRID - 1, ZS - BOX + 1, ZS).astype(jnp.int32)
    local = jax.random.randint(key_depth, (ATOMS,), 0, top).astype(jnp.int32)
    depth = slab * ZS + local
    row_start = jax.random.randint(key_row, (ATOMS,), 0, NY - BOX + 1).astype(jnp.int32)
    column_start = jax.random.randint(key_column, (ATOMS,), 0, NX - BOX + 1).astype(jnp.int32)
    stacked = jnp.stack([depth, row_start, column_start]).astype(jnp.int32)
    order = jax.random.permutation(key_atoms, ATOMS)
    return stacked[:, order]


def with_ends(drawn, stream_key, low, high):
    spot = [jax.random.randint(jax.random.fold_in(stream_key, axis), (), 0, length) for axis, length in enumerate(drawn.shape)]
    main_axis = drawn.shape.index(max(drawn.shape))
    neighbour = spot[:main_axis] + [(spot[main_axis] + 1) % drawn.shape[main_axis]] + spot[main_axis + 1:]
    return drawn.at[tuple(spot)].set(low).at[tuple(neighbour)].set(high)


def steps_of(stream_key, shape, pieces, smallest, top_value):
    level, own = 1.0, jax.random.fold_in(stream_key, 6)
    for axis_at, parts in pieces:
        draws = jnp.exp(jax.random.uniform(jax.random.fold_in(own, axis_at), (parts,), jnp.float32, smallest / len(pieces), top_value / len(pieces)))
        level = level * jnp.repeat(draws, shape[axis_at] // parts).reshape([-1 if axis == axis_at else 1 for axis in range(len(shape))])
    return level


def normal_values(key, dims, width, bound, pieces=(), kind=jnp.bfloat16):
    result = width * jax.random.normal(key, dims, jnp.float32)
    if pieces:
        result = result * steps_of(key, dims, pieces, -0.22, 0.18)
    return jnp.clip(result, -bound, bound).astype(kind)


def setup_inputs(seed: int = 0) -> dict:
    streams_of = jax.random.split(jax.random.key(seed), 5)
    coefficients = normal_values(streams_of[0], (ATOMS, NPROJ, BANDS), BANDS ** -0.5, 0.125, ((0, 8), (2, 4)))
    occupation = with_ends(jax.random.randint(streams_of[1], (BANDS,), 0, 9), jax.random.fold_in(streams_of[1], 1), 0, 8).astype(jnp.int32)
    shapes = normal_values(streams_of[2], (NPAIR, BOX * BOX * BOX), NPROJ ** -0.5, 1.5)
    corners = draw_corners(jax.random.fold_in(streams_of[4], 71), 0)
    return {"coefficients": coefficients, "occupation": occupation, "shapes": shapes, "corners": corners}


def fold_table(count):
    table = np.zeros((count * count, count * (count + 1) // 2), np.float32)
    column = 0
    for first in range(count):
        for second in range(first, count):
            table[first * count + second, column] = 1.0
            table[second * count + first, column] = 1.0
            column = column + 1
    return table


def occupancy(coefficients, occupation):
    weighted = coefficients.astype(jnp.float32) * (occupation.astype(jnp.float32) * 0.25)[None, None, :]
    full = jnp.einsum("aib,ajb->aij", weighted, coefficients.astype(jnp.float32), precision=lax.Precision.HIGHEST)
    count = coefficients.shape[1]
    flat = full.reshape(coefficients.shape[0], count * count)
    return jnp.dot(flat, jnp.asarray(fold_table(count)), precision=lax.Precision.HIGHEST)


def reference(coefficients, occupation, shapes, corners):
    packed = occupancy(coefficients, occupation).astype(jnp.bfloat16)
    start_grid = jnp.zeros((NZ, NY, NX), jnp.float32)

    def place(grid, item):
        row, corner = item
        box = jnp.dot(row[None, :], shapes, preferred_element_type=jnp.float32).reshape(BOX, BOX, BOX)
        start = (corner[0], corner[1], corner[2])
        region = lax.dynamic_slice(grid, start, (BOX, BOX, BOX))
        return lax.dynamic_update_slice(grid, region + box, start), None

    density, unused = lax.scan(place, start_grid, (packed, corners.T.astype(jnp.int32)))
    return density
```

```python
import functools

import jax
import jax.numpy as jnp
import numpy as np
from jax import lax
from jax.experimental import pallas as pl
from jax.experimental.pallas import tpu as pltpu
from jax.sharding import PartitionSpec as P

BOX = 32
ZS = 32
NY = 288
NX = 288
LANES = 128
STEP = LANES - BOX
GROUP = 8
UNROLL = 2


def fold_table(count):
    table = np.zeros((count * count, count * (count + 1) // 2), np.float32)
    column = 0
    for first in range(count):
        for second in range(first, count):
            table[first * count + second, column] = 1.0
            table[second * count + first, column] = 1.0
            column = column + 1
    return table


def occupancy(coefficients, occupation):
    weight = occupation.astype(jnp.float32) * 0.25
    weighted = coefficients.astype(jnp.float32) * weight[None, None, :]
    high = weighted.astype(jnp.bfloat16)
    low = (weighted - high.astype(jnp.float32)).astype(jnp.bfloat16)
    pairs = functools.partial(jnp.einsum, "aib,ajb->aij", preferred_element_type=jnp.float32)
    full = pairs(high, coefficients) + pairs(low, coefficients)
    count = coefficients.shape[1]
    flat = full.reshape(coefficients.shape[0], count * count)
    return jnp.dot(flat, jnp.asarray(fold_table(count)), precision=lax.Precision.HIGHEST)


WINDOWS = (NX - BOX) // STEP + 1
QUARTER = NY // 4
PLANES = ZS + 2 * GROUP
TILES = -(-NX // LANES)
TAIL = NX % LANES


def place_kernel(
    slots, stride, packed_ref, corners_ref, shapes_ref, out_ref,
    shp, sel, boxes, acc, stage, tail, item_a, item_b, shape_sem, out_sem,
):
    slab = lax.axis_index("grid")
    atoms = packed_ref.shape[0]
    columns = shapes_ref.shape[1]
    pieces = BOX // GROUP
    piece = columns // pieces

    def shape_copy(j):
        cols = pl.ds(j * piece, piece)
        return pltpu.make_async_copy(shapes_ref.at[:, cols], shp.at[:, cols], shape_sem.at[j])

    for j in range(pieces):
        shape_copy(j).start()

    zero_rows = acc.shape[0] // atoms
    zero = jnp.zeros((8, LANES), jnp.float32)

    def add_item(count, source, window, row, turn):
        item_a[count] = source + window * 65536
        item_b[count] = row + turn * 512

    def list_atom(a, carry):
        own_count, below_count, count = carry
        for i in range(zero_rows // 8):
            acc[pl.ds(pl.multiple_of(a * zero_rows, 8) + 8 * i, 8), :] = zero
        depth = corners_ref[0, a]
        owner = depth // ZS
        local = depth - owner * ZS
        own = owner == slab
        below = owner == slab - 1
        row = corners_ref[1, a]
        column = corners_ref[2, a]
        window = column // STEP
        turn = lax.rem(column - window * STEP + 32 * row, LANES)
        slot = jnp.where(own, own_count, jnp.where(below, slots + below_count, 2 * slots))
        sel[pl.ds(slot, 1), :] = packed_ref[pl.ds(a, 1), :]
        first = jnp.where(own, 0, jnp.where(below, (BOX - local) // GROUP, pieces))
        last = jnp.where(own, (BOX - local + GROUP - 1) // GROUP, pieces)
        shift = jnp.where(own, local, local - ZS) + GROUP

        def emit(j, at):
            plane = shift + j * GROUP
            add_item(at, slot + j * GROUP * 8 * stride, plane * WINDOWS + window, row, turn)
            return at + 1

        count = lax.fori_loop(first, last, emit, count)
        return (
            own_count + own.astype(jnp.int32),
            below_count + below.astype(jnp.int32),
            count,
        )

    start = jnp.int32(0)
    own_count, below_count, count = lax.fori_loop(0, atoms, list_atom, (start, start, start))
    for extra in range(UNROLL - 1):
        add_item(count + extra, 0, 0, 0, 0)

    rows = sel[: 2 * slots, :].astype(jnp.bfloat16)
    span = 1024
    for j in range(pieces):
        shape_copy(j).wait()

        def multiply(s, carry):
            at = pl.multiple_of(j * piece + s * span, span)
            product = jnp.dot(rows, shp[:, pl.ds(at, span)], preferred_element_type=jnp.float32)
            for c in range(span // LANES):
                target = (at // LANES + c) * stride
                boxes[pl.ds(target, 2 * slots), :] = product[:, c * LANES : (c + 1) * LANES]
            return carry

        lax.fori_loop(0, piece // span, multiply, 0)

    lane = lax.broadcasted_iota(jnp.int32, (8, LANES), 1)

    def place_one(n):
        word_a = item_a[n]
        word_b = item_b[n]
        source = lax.bitwise_and(word_a, 65535)
        base = lax.shift_right_logical(word_a, 16) * NY
        row = lax.bitwise_and(word_b, 511)
        turn = lax.shift_right_logical(word_b, 9)
        part = lax.shift_right_logical(lax.bitwise_and(lane - turn, LANES - 1), 5)
        masks = [part == g for g in range(4)]
        starts = [
            base + lax.bitwise_and(row + g, 3) * QUARTER + lax.shift_right_logical(row + g, 2)
            for g in range(4)
        ]
        turned = [
            pltpu.roll(boxes[pl.ds(source + k * 8 * stride, 8, stride=stride), :], turn, 1)
            for k in range(GROUP)
        ]
        sums = []
        for k in range(GROUP):
            for g in range(4):
                at = starts[g] + k * WINDOWS * NY
                sums.append((at, acc[pl.ds(at, 8), :] + jnp.where(masks[g], turned[k], 0.0)))
        for at, value in sums:
            acc[pl.ds(at, 8), :] = value

    def place(step, carry):
        for u in range(UNROLL):
            place_one(step * UNROLL + u)
        return carry

    lax.fori_loop(0, (count + UNROLL - 1) // UNROLL, place, 0)

    def out_copy(z, v):
        width = min(LANES, NX - v * LANES)
        slot = lax.rem(z, 2)
        return pltpu.make_async_copy(
            stage.at[slot, v] if width == LANES else tail.at[slot],
            out_ref.at[z, :, pl.ds(v * LANES, width)],
            out_sem.at[slot, v],
        )

    def finish(z, carry):
        @pl.when(z >= 2)
        def _():
            for v in range(TILES):
                out_copy(z - 2, v).wait()

        slot = lax.rem(z, 2)
        base = (z + GROUP) * WINDOWS * NY
        for r in range(4):
            for i in range(QUARTER // 8):
                parts = []
                for t in range(WINDOWS):
                    at = pl.multiple_of(base, 8) + t * NY + r * QUARTER + 8 * i
                    amount = (STEP * t - 32 * r) % LANES
                    value = acc[pl.ds(at, 8), :]
                    parts.append(pltpu.roll(value, amount, 1) if amount else value)
                for v in range(TILES):
                    total = None
                    for t in range(WINDOWS):
                        low = max(STEP * t - LANES * v, 0)
                        high = min(STEP * t + LANES - LANES * v, LANES)
                        if low >= min(high, NX - LANES * v):
                            continue
                        value = parts[t]
                        if low > 0:
                            value = jnp.where(lane >= low, value, 0.0)
                        elif high < LANES:
                            value = jnp.where(lane < high, value, 0.0)
                        total = value if total is None else total + value
                    stage[slot, v, pl.ds(r + 32 * i, 8, stride=4), :] = total
        if TAIL:
            tail[slot] = stage[slot, TILES - 1, :, :TAIL]
        for v in range(TILES):
            out_copy(z, v).start()
        return carry

    lax.fori_loop(0, ZS, finish, 0)
    for z in range(ZS - 2, ZS):
        for v in range(TILES):
            out_copy(jnp.int32(z), v).wait()


def place_boxes(packed, corners, shapes, slots):
    stride = 2 * slots + 1
    count, columns = shapes.shape
    atoms = packed.shape[0]
    items = 2 * slots * (BOX // GROUP) + UNROLL
    any_space = pl.BlockSpec(memory_space=pl.ANY)
    return pl.pallas_call(
        functools.partial(place_kernel, slots, stride),
        out_shape=jax.ShapeDtypeStruct((ZS, NY, NX), jnp.float32),
        in_specs=[
            pl.BlockSpec(memory_space=pltpu.VMEM),
            pl.BlockSpec(memory_space=pltpu.SMEM),
            any_space,
        ],
        out_specs=any_space,
        scratch_shapes=[
            pltpu.VMEM((count, columns), jnp.bfloat16),
            pltpu.VMEM((2 * slots + 8, count), jnp.float32),
            pltpu.VMEM((columns // LANES * stride + 8, LANES), jnp.float32),
            pltpu.VMEM((-(-PLANES * WINDOWS * NY // (8 * atoms)) * 8 * atoms, LANES), jnp.float32),
            pltpu.VMEM((2, TILES, NY, LANES), jnp.float32),
            pltpu.VMEM((2, NY, max(TAIL, 1)), jnp.float32),
            pltpu.SMEM((items,), jnp.int32),
            pltpu.SMEM((items,), jnp.int32),
            pltpu.SemaphoreType.DMA((BOX // GROUP,)),
            pltpu.SemaphoreType.DMA((2, TILES)),
        ],
        compiler_params=pltpu.CompilerParams(vmem_limit_bytes=63 * 1024 * 1024),
    )(packed, corners, shapes)


def body(coefficients, occupation, shapes, corners):
    partial_value = occupancy(coefficients, occupation)
    every = lax.all_gather(partial_value, ("band", "grid"), axis=0, tiled=False)
    bands = lax.axis_size("band")
    summed = every.reshape(bands, -1, partial_value.shape[1]).sum(axis=0)
    packed = summed.astype(jnp.bfloat16).astype(jnp.float32)
    return place_boxes(packed, corners, shapes, 2 * coefficients.shape[0])


def solution(mesh):
    placed = (P("grid", None, "band"), P("band"), P(), P())
    return jax.shard_map(
        body, mesh=mesh, in_specs=placed, out_specs=P("grid", None, None), check_vma=False
    )
```

```python
import functools

import jax
import jax.numpy as jnp
import numpy as np
from jax import lax
from jax.experimental import pallas as pl
from jax.experimental.pallas import tpu as pltpu
from jax.sharding import PartitionSpec as P

BOX = 32
ZS = 32
NY = 288
NX = 288
LANES = 128
STEP = LANES - BOX
GROUP = 8
UNROLL = 2


def fold_table(count):
    table = np.zeros((count * count, count * (count + 1) // 2), np.float32)
    column = 0
    for first in range(count):
        for second in range(first, count):
            table[first * count + second, column] = 1.0
            table[second * count + first, column] = 1.0
            column = column + 1
    return table


def occupancy(coefficients, occupation):
    weight = occupation.astype(jnp.float32) * 0.25
    weighted = coefficients.astype(jnp.float32) * weight[None, None, :]
    high = lax.reduce_precision(weighted, 8, 7)
    low = (weighted - high).astype(jnp.bfloat16)
    high = high.astype(jnp.bfloat16)
    pairs = functools.partial(jnp.einsum, "aib,ajb->aij", preferred_element_type=jnp.float32)
    full = pairs(high, coefficients) + pairs(low, coefficients)
    count = coefficients.shape[1]
    flat = full.reshape(coefficients.shape[0], count * count)
    return jnp.dot(flat, jnp.asarray(fold_table(count)), precision=lax.Precision.HIGHEST)


WINDOWS = (NX - BOX) // STEP + 1
QUARTER = NY // 4
PLANES = ZS + 2 * GROUP
TILES = -(-NX // LANES)
TAIL = NX % LANES


def place_kernel(
    slots, stride, packed_ref, corners_ref, shapes_ref, out_ref,
    shp, sel, boxes, acc, stage, tail, item_a, item_b, shape_sem, out_sem,
):
    slab = lax.axis_index("grid")
    atoms = packed_ref.shape[0]
    columns = shapes_ref.shape[1]
    pieces = BOX // GROUP
    piece = columns // pieces

    def shape_copy(j):
        cols = pl.ds(j * piece, piece)
        return pltpu.make_async_copy(shapes_ref.at[:, cols], shp.at[:, cols], shape_sem.at[j])

    for j in range(pieces):
        shape_copy(j).start()

    zero_rows = acc.shape[0] // atoms
    zero = jnp.zeros((8, LANES), jnp.float32)

    def add_item(count, source, window, row, turn):
        item_a[count] = source + window * 65536
        item_b[count] = row + turn * 512

    def list_atom(a, carry):
        own_count, below_count, count = carry
        for i in range(zero_rows // 8):
            acc[pl.ds(pl.multiple_of(a * zero_rows, 8) + 8 * i, 8), :] = zero
        depth = corners_ref[0, a]
        owner = depth // ZS
        local = depth - owner * ZS
        own = owner == slab
        below = owner == slab - 1
        row = corners_ref[1, a]
        column = corners_ref[2, a]
        window = column // STEP
        turn = lax.rem(column - window * STEP + 32 * row, LANES)
        slot = jnp.where(own, own_count, jnp.where(below, slots + below_count, 2 * slots))
        sel[pl.ds(slot, 1), :] = packed_ref[pl.ds(a, 1), :]
        first = jnp.where(own, 0, jnp.where(below, (BOX - local) // GROUP, pieces))
        last = jnp.where(own, (BOX - local + GROUP - 1) // GROUP, pieces)
        shift = jnp.where(own, local, local - ZS) + GROUP

        def emit(j, at):
            plane = shift + j * GROUP
            add_item(at, slot + j * GROUP * 8 * stride, plane * WINDOWS + window, row, turn)
            return at + 1

        count = lax.fori_loop(first, last, emit, count)
        return (
            own_count + own.astype(jnp.int32),
            below_count + below.astype(jnp.int32),
            count,
        )

    start = jnp.int32(0)
    own_count, below_count, count = lax.fori_loop(0, atoms, list_atom, (start, start, start))
    for extra in range(UNROLL - 1):
        add_item(count + extra, 0, 0, 0, 0)

    rows = sel[: 2 * slots, :].astype(jnp.bfloat16)
    span = 1024
    for j in range(pieces):
        shape_copy(j).wait()

        def multiply(s, carry):
            at = pl.multiple_of(j * piece + s * span, span)
            product = jnp.dot(rows, shp[:, pl.ds(at, span)], preferred_element_type=jnp.float32)
            for c in range(span // LANES):
                target = (at // LANES + c) * stride
                boxes[pl.ds(target, 2 * slots), :] = product[:, c * LANES : (c + 1) * LANES]
            return carry

        lax.fori_loop(0, piece // span, multiply, 0)

    lane = lax.broadcasted_iota(jnp.int32, (8, LANES), 1)

    def place_one(n):
        word_a = item_a[n]
        word_b = item_b[n]
        source = lax.bitwise_and(word_a, 65535)
        base = lax.shift_right_logical(word_a, 16) * NY
        row = lax.bitwise_and(word_b, 511)
        turn = lax.shift_right_logical(word_b, 9)
        part = lax.shift_right_logical(lax.bitwise_and(lane - turn, LANES - 1), 5)
        masks = [part == g for g in range(4)]
        starts = [
            base + lax.bitwise_and(row + g, 3) * QUARTER + lax.shift_right_logical(row + g, 2)
            for g in range(4)
        ]
        turned = [
            pltpu.roll(boxes[pl.ds(source + k * 8 * stride, 8, stride=stride), :], turn, 1)
            for k in range(GROUP)
        ]
        sums = []
        for k in range(GROUP):
            for g in range(4):
                at = starts[g] + k * WINDOWS * NY
                sums.append((at, acc[pl.ds(at, 8), :] + jnp.where(masks[g], turned[k], 0.0)))
        for at, value in sums:
            acc[pl.ds(at, 8), :] = value

    def place(step, carry):
        for u in range(UNROLL):
            place_one(step * UNROLL + u)
        return carry

    lax.fori_loop(0, (count + UNROLL - 1) // UNROLL, place, 0)

    def out_copy(z, v):
        width = min(LANES, NX - v * LANES)
        slot = lax.rem(z, 2)
        return pltpu.make_async_copy(
            stage.at[slot, v] if width == LANES else tail.at[slot],
            out_ref.at[z, :, pl.ds(v * LANES, width)],
            out_sem.at[slot, v],
        )

    def finish(z, carry):
        @pl.when(z >= 2)
        def _():
            for v in range(TILES):
                out_copy(z - 2, v).wait()

        slot = lax.rem(z, 2)
        base = (z + GROUP) * WINDOWS * NY
        for r in range(4):
            for i in range(QUARTER // 8):
                parts = []
                for t in range(WINDOWS):
                    at = pl.multiple_of(base, 8) + t * NY + r * QUARTER + 8 * i
                    amount = (STEP * t - 32 * r) % LANES
                    value = acc[pl.ds(at, 8), :]
                    parts.append(pltpu.roll(value, amount, 1) if amount else value)
                for v in range(TILES):
                    total = None
                    for t in range(WINDOWS):
                        low = max(STEP * t - LANES * v, 0)
                        high = min(STEP * t + LANES - LANES * v, LANES)
                        if low >= min(high, NX - LANES * v):
                            continue
                        value = parts[t]
                        if low > 0:
                            value = jnp.where(lane >= low, value, 0.0)
                        elif high < LANES:
                            value = jnp.where(lane < high, value, 0.0)
                        total = value if total is None else total + value
                    stage[slot, v, pl.ds(r + 32 * i, 8, stride=4), :] = total
        if TAIL:
            tail[slot] = stage[slot, TILES - 1, :, :TAIL]
        for v in range(TILES):
            out_copy(z, v).start()
        return carry

    lax.fori_loop(0, ZS, finish, 0)
    for z in range(ZS - 2, ZS):
        for v in range(TILES):
            out_copy(jnp.int32(z), v).wait()


def place_boxes(packed, corners, shapes, slots):
    stride = 2 * slots + 1
    count, columns = shapes.shape
    atoms = packed.shape[0]
    items = 2 * slots * (BOX // GROUP) + UNROLL
    any_space = pl.BlockSpec(memory_space=pl.ANY)
    return pl.pallas_call(
        functools.partial(place_kernel, slots, stride),
        out_shape=jax.ShapeDtypeStruct((ZS, NY, NX), jnp.float32),
        in_specs=[
            pl.BlockSpec(memory_space=pltpu.VMEM),
            pl.BlockSpec(memory_space=pltpu.SMEM),
            any_space,
        ],
        out_specs=any_space,
        scratch_shapes=[
            pltpu.VMEM((count, columns), jnp.bfloat16),
            pltpu.VMEM((2 * slots + 8, count), jnp.float32),
            pltpu.VMEM((columns // LANES * stride + 8, LANES), jnp.float32),
            pltpu.VMEM((-(-PLANES * WINDOWS * NY // (8 * atoms)) * 8 * atoms, LANES), jnp.float32),
            pltpu.VMEM((2, TILES, NY, LANES), jnp.float32),
            pltpu.VMEM((2, NY, max(TAIL, 1)), jnp.float32),
            pltpu.SMEM((items,), jnp.int32),
            pltpu.SMEM((items,), jnp.int32),
            pltpu.SemaphoreType.DMA((BOX // GROUP,)),
            pltpu.SemaphoreType.DMA((2, TILES)),
        ],
        compiler_params=pltpu.CompilerParams(vmem_limit_bytes=63 * 1024 * 1024),
    )(packed, corners, shapes)


def share_kernel(bands, slabs, part_ref, out_ref, parts, mine, rows, send_a, recv_a, send_b, recv_b):
    band = lax.axis_index("band")
    slab = lax.axis_index("grid")
    barrier = pltpu.get_barrier_semaphore()
    mesh_id = pl.DeviceIdType.MESH

    def band_peer(d):
        return (lax.rem(band + d, bands), slab)

    def slab_peer(d):
        return (band, lax.rem(slab + d, slabs))

    peers = [band_peer(d) for d in range(1, bands)] + [slab_peer(d) for d in range(1, slabs)]
    for peer in peers:
        pl.semaphore_signal(barrier, inc=1, device_id=peer, device_id_type=mesh_id)
    pl.semaphore_wait(barrier, len(peers))

    copies = []
    for d in range(1, bands):
        copy = pltpu.make_async_remote_copy(
            src_ref=part_ref, dst_ref=parts.at[band], send_sem=send_a.at[d - 1],
            recv_sem=recv_a.at[d - 1], device_id=band_peer(d), device_id_type=mesh_id,
        )
        copy.start()
        copies.append(copy)
    parts[band] = part_ref[...]
    for copy in copies:
        copy.wait()
    total = parts[0]
    for b in range(1, bands):
        total = total + parts[b]
    packed = total.astype(jnp.bfloat16)
    mine[...] = packed
    copies = []
    for d in range(1, slabs):
        copy = pltpu.make_async_remote_copy(
            src_ref=mine, dst_ref=rows.at[slab], send_sem=send_b.at[d - 1],
            recv_sem=recv_b.at[d - 1], device_id=slab_peer(d), device_id_type=mesh_id,
        )
        copy.start()
        copies.append(copy)
    rows[slab] = packed
    for copy in copies:
        copy.wait()
    out_ref[...] = rows[...].astype(jnp.float32)


def share(part, bands, slabs):
    count, width = part.shape
    vmem = pl.BlockSpec(memory_space=pltpu.VMEM)
    return pl.pallas_call(
        functools.partial(share_kernel, bands, slabs),
        out_shape=jax.ShapeDtypeStruct((slabs, count, width), jnp.float32),
        in_specs=[vmem],
        out_specs=vmem,
        scratch_shapes=[
            pltpu.VMEM((bands, count, width), jnp.float32),
            pltpu.VMEM((count, width), jnp.bfloat16),
            pltpu.VMEM((slabs, count, width), jnp.bfloat16),
            pltpu.SemaphoreType.DMA((bands - 1,)),
            pltpu.SemaphoreType.DMA((bands - 1,)),
            pltpu.SemaphoreType.DMA((slabs - 1,)),
            pltpu.SemaphoreType.DMA((slabs - 1,)),
        ],
        compiler_params=pltpu.CompilerParams(collective_id=0, has_side_effects=True),
    )(part)


def body(coefficients, occupation, shapes, corners):
    part = occupancy(coefficients, occupation)
    packed = share(part, lax.axis_size("band"), lax.axis_size("grid"))
    packed = packed.reshape(-1, part.shape[1])
    return place_boxes(packed, corners, shapes, 2 * coefficients.shape[0])


def solution(mesh):
    placed = (P("grid", None, "band"), P("band"), P(), P())
    return jax.shard_map(
        body, mesh=mesh, in_specs=placed, out_specs=P("grid", None, None), check_vma=False
    )
```

```python
import functools

import jax
import jax.numpy as jnp
import numpy as np
from jax import lax
from jax.experimental import pallas as pl
from jax.experimental.pallas import tpu as pltpu
from jax.sharding import PartitionSpec as P

BOX = 32
ZS = 32
NY = 288
NX = 288
LANES = 128
STEP = LANES - BOX
GROUP = 8
UNROLL = 8
DEPTH = 4


def fold_table(count):
    table = np.zeros((count * count, count * (count + 1) // 2), np.float32)
    column = 0
    for first in range(count):
        for second in range(first, count):
            table[first * count + second, column] = 1.0
            table[second * count + first, column] = 1.0
            column = column + 1
    return table


def occupancy(coefficients, occupation):
    weight = occupation.astype(jnp.float32) * 0.25
    weighted = coefficients.astype(jnp.float32) * weight[None, None, :]
    high = lax.reduce_precision(weighted, 8, 7)
    low = (weighted - high).astype(jnp.bfloat16)
    high = high.astype(jnp.bfloat16)
    pairs = functools.partial(jnp.einsum, "aib,ajb->aij", preferred_element_type=jnp.float32)
    full = pairs(high, coefficients) + pairs(low, coefficients)
    count = coefficients.shape[1]
    flat = full.reshape(coefficients.shape[0], count * count)
    return jnp.dot(flat, jnp.asarray(fold_table(count)), precision=lax.Precision.HIGHEST)


WINDOWS = (NX - BOX) // STEP + 1
QUARTER = NY // 4
PLANES = ZS + 2 * GROUP
TILES = -(-NX // LANES)
TAIL = NX % LANES


def place_kernel(
    slots, stride, packed_ref, corners_ref, shapes_ref, out_ref,
    shp, sel, boxes, acc, stage, tail, item_a, item_b, shape_sem, out_sem,
):
    slab = lax.axis_index("grid")
    atoms = packed_ref.shape[0]
    columns = shapes_ref.shape[1]
    pieces = BOX // GROUP
    piece = columns // pieces

    def shape_copy(j):
        cols = pl.ds(j * piece, piece)
        return pltpu.make_async_copy(shapes_ref.at[:, cols], shp.at[:, cols], shape_sem.at[j])

    for j in range(pieces):
        shape_copy(j).start()

    zero_rows = acc.shape[0] // atoms
    zero = jnp.zeros((8, LANES), jnp.float32)

    def add_item(count, source, window, row, turn):
        item_a[count] = source + window * 65536
        item_b[count] = row + turn * 512

    def list_atom(a, carry):
        own_count, below_count, count = carry
        for i in range(zero_rows // 8):
            acc[pl.ds(pl.multiple_of(a * zero_rows, 8) + 8 * i, 8), :] = zero
        depth = corners_ref[0, a]
        owner = lax.shift_right_logical(depth, ZS.bit_length() - 1)
        local = depth - owner * ZS
        own = owner == slab
        below = owner == slab - 1
        row = corners_ref[1, a]
        column = corners_ref[2, a]
        window = jnp.int32(0)
        for t in range(1, WINDOWS):
            window = window + (column >= t * STEP).astype(jnp.int32)
        turn = lax.bitwise_and(column - window * STEP + 32 * row, LANES - 1)
        slot = jnp.where(own, own_count, jnp.where(below, slots + below_count, 2 * slots))
        sel[pl.ds(slot, 1), :] = packed_ref[pl.ds(a, 1), :]
        edge = jnp.where(own, BOX - local + GROUP - 1, BOX - local)
        edge = lax.shift_right_logical(edge, GROUP.bit_length() - 1)
        shift = jnp.where(own, local, local - ZS) + GROUP
        head = slot + (shift * WINDOWS + window) * 65536
        tail_word = row + turn * 512
        near = own.astype(jnp.int32)
        far = below.astype(jnp.int32)
        for j in range(pieces):
            item_a[count] = head + j * GROUP * (8 * stride + WINDOWS * 65536)
            item_b[count] = tail_word
            count = count + jnp.where(edge > j, near, far)
        return (
            own_count + own.astype(jnp.int32),
            below_count + below.astype(jnp.int32),
            count,
        )

    start = jnp.int32(0)
    own_count, below_count, count = lax.fori_loop(0, atoms, list_atom, (start, start, start))
    for extra in range(UNROLL - 1):
        add_item(count + extra, 0, 0, 0, 0)

    rows = sel[: 2 * slots, :].astype(jnp.bfloat16)
    span = 4096
    for j in range(pieces):
        shape_copy(j).wait()

        def multiply(s, carry):
            at = pl.multiple_of(j * piece + s * span, span)
            product = jnp.dot(rows, shp[:, pl.ds(at, span)], preferred_element_type=jnp.float32)
            for c in range(span // LANES):
                target = (at // LANES + c) * stride
                boxes[pl.ds(target, 2 * slots), :] = product[:, c * LANES : (c + 1) * LANES]
            return carry

        lax.fori_loop(0, piece // span, multiply, 0)

    lane = lax.broadcasted_iota(jnp.int32, (8, LANES), 1)

    def place_one(n):
        word_a = item_a[n]
        word_b = item_b[n]
        source = lax.bitwise_and(word_a, 65535)
        base = lax.shift_right_logical(word_a, 16) * NY
        row = lax.bitwise_and(word_b, 511)
        turn = lax.shift_right_logical(word_b, 9)
        part = lax.shift_right_logical(lax.bitwise_and(lane - turn, LANES - 1), 5)
        masks = [part == g for g in range(4)]
        starts = [
            base + lax.bitwise_and(row + g, 3) * QUARTER + lax.shift_right_logical(row + g, 2)
            for g in range(4)
        ]
        turned = [
            pltpu.roll(boxes[pl.ds(source + k * 8 * stride, 8, stride=stride), :], turn, 1)
            for k in range(GROUP)
        ]
        sums = []
        for k in range(GROUP):
            for g in range(4):
                at = starts[g] + k * WINDOWS * NY
                sums.append((at, acc[pl.ds(at, 8), :] + jnp.where(masks[g], turned[k], 0.0)))
        for at, value in sums:
            acc[pl.ds(at, 8), :] = value

    def place(step, carry):
        for u in range(UNROLL):
            place_one(step * UNROLL + u)
        return carry

    lax.fori_loop(0, (count + UNROLL - 1) // UNROLL, place, 0)

    def out_copy(z, v):
        width = min(LANES, NX - v * LANES)
        slot = lax.rem(z, DEPTH)
        return pltpu.make_async_copy(
            stage.at[slot, v] if width == LANES else tail.at[slot],
            out_ref.at[z, :, pl.ds(v * LANES, width)],
            out_sem.at[slot, v],
        )

    def finish(z, carry):
        @pl.when(z >= DEPTH)
        def _():
            for v in range(TILES):
                out_copy(z - DEPTH, v).wait()

        slot = lax.rem(z, DEPTH)
        base = (z + GROUP) * WINDOWS * NY
        for r in range(4):
            for i in range(QUARTER // 8):
                parts = []
                for t in range(WINDOWS):
                    at = pl.multiple_of(base, 8) + t * NY + r * QUARTER + 8 * i
                    amount = (STEP * t - 32 * r) % LANES
                    value = acc[pl.ds(at, 8), :]
                    parts.append(pltpu.roll(value, amount, 1) if amount else value)
                for v in range(TILES):
                    total = None
                    for t in range(WINDOWS):
                        low = max(STEP * t - LANES * v, 0)
                        high = min(STEP * t + LANES - LANES * v, LANES)
                        if low >= min(high, NX - LANES * v):
                            continue
                        value = parts[t]
                        if low > 0:
                            value = jnp.where(lane >= low, value, 0.0)
                        elif high < LANES:
                            value = jnp.where(lane < high, value, 0.0)
                        total = value if total is None else total + value
                    stage[slot, v, pl.ds(r + 32 * i, 8, stride=4), :] = total
        if TAIL:
            tail[slot] = stage[slot, TILES - 1, :, :TAIL]
        for v in range(TILES):
            out_copy(z, v).start()
        return carry

    lax.fori_loop(0, ZS, finish, 0)
    for z in range(ZS - DEPTH, ZS):
        for v in range(TILES):
            out_copy(jnp.int32(z), v).wait()


def place_boxes(packed, corners, shapes, slots):
    stride = 2 * slots + 1
    count, columns = shapes.shape
    atoms = packed.shape[0]
    items = 2 * slots * (BOX // GROUP) + UNROLL + 1
    any_space = pl.BlockSpec(memory_space=pl.ANY)
    return pl.pallas_call(
        functools.partial(place_kernel, slots, stride),
        out_shape=jax.ShapeDtypeStruct((ZS, NY, NX), jnp.float32),
        in_specs=[
            pl.BlockSpec(memory_space=pltpu.VMEM),
            pl.BlockSpec(memory_space=pltpu.SMEM),
            any_space,
        ],
        out_specs=any_space,
        scratch_shapes=[
            pltpu.VMEM((count, columns), jnp.bfloat16),
            pltpu.VMEM((2 * slots + 8, count), jnp.float32),
            pltpu.VMEM((columns // LANES * stride + 8, LANES), jnp.float32),
            pltpu.VMEM((-(-PLANES * WINDOWS * NY // (8 * atoms)) * 8 * atoms, LANES), jnp.float32),
            pltpu.VMEM((DEPTH, TILES, NY, LANES), jnp.float32),
            pltpu.VMEM((DEPTH, NY, max(TAIL, 1)), jnp.float32),
            pltpu.SMEM((items,), jnp.int32),
            pltpu.SMEM((items,), jnp.int32),
            pltpu.SemaphoreType.DMA((BOX // GROUP,)),
            pltpu.SemaphoreType.DMA((DEPTH, TILES)),
        ],
        compiler_params=pltpu.CompilerParams(vmem_limit_bytes=63 * 1024 * 1024),
    )(packed, corners, shapes)


def share_kernel(bands, slabs, part_ref, out_ref, parts, mine, rows, send_a, recv_a, send_b, recv_b):
    band = lax.axis_index("band")
    slab = lax.axis_index("grid")
    barrier = pltpu.get_barrier_semaphore()
    mesh_id = pl.DeviceIdType.MESH

    def band_peer(d):
        return (lax.rem(band + d, bands), slab)

    def slab_peer(d):
        return (band, lax.rem(slab + d, slabs))

    peers = [band_peer(d) for d in range(1, bands)] + [slab_peer(d) for d in range(1, slabs)]
    for peer in peers:
        pl.semaphore_signal(barrier, inc=1, device_id=peer, device_id_type=mesh_id)
    pl.semaphore_wait(barrier, len(peers))

    copies = []
    for d in range(1, bands):
        copy = pltpu.make_async_remote_copy(
            src_ref=part_ref, dst_ref=parts.at[band], send_sem=send_a.at[d - 1],
            recv_sem=recv_a.at[d - 1], device_id=band_peer(d), device_id_type=mesh_id,
        )
        copy.start()
        copies.append(copy)
    parts[band] = part_ref[...]
    for copy in copies:
        copy.wait()
    total = parts[0]
    for b in range(1, bands):
        total = total + parts[b]
    packed = total.astype(jnp.bfloat16)
    mine[...] = packed
    copies = []
    for d in range(1, slabs):
        copy = pltpu.make_async_remote_copy(
            src_ref=mine, dst_ref=rows.at[slab], send_sem=send_b.at[d - 1],
            recv_sem=recv_b.at[d - 1], device_id=slab_peer(d), device_id_type=mesh_id,
        )
        copy.start()
        copies.append(copy)
    rows[slab] = packed
    for copy in copies:
        copy.wait()
    out_ref[...] = rows[...].astype(jnp.float32)


def share(part, bands, slabs):
    count, width = part.shape
    vmem = pl.BlockSpec(memory_space=pltpu.VMEM)
    return pl.pallas_call(
        functools.partial(share_kernel, bands, slabs),
        out_shape=jax.ShapeDtypeStruct((slabs, count, width), jnp.float32),
        in_specs=[vmem],
        out_specs=vmem,
        scratch_shapes=[
            pltpu.VMEM((bands, count, width), jnp.float32),
            pltpu.VMEM((count, width), jnp.bfloat16),
            pltpu.VMEM((slabs, count, width), jnp.bfloat16),
            pltpu.SemaphoreType.DMA((bands - 1,)),
            pltpu.SemaphoreType.DMA((bands - 1,)),
            pltpu.SemaphoreType.DMA((slabs - 1,)),
            pltpu.SemaphoreType.DMA((slabs - 1,)),
        ],
        compiler_params=pltpu.CompilerParams(collective_id=0, has_side_effects=True),
    )(part)


def body(coefficients, occupation, shapes, corners):
    part = occupancy(coefficients, occupation)
    packed = share(part, lax.axis_size("band"), lax.axis_size("grid"))
    packed = packed.reshape(-1, part.shape[1])
    return place_boxes(packed, corners, shapes, 2 * coefficients.shape[0])


def solution(mesh):
    placed = (P("grid", None, "band"), P("band"), P(), P())
    return jax.shard_map(
        body, mesh=mesh, in_specs=placed, out_specs=P("grid", None, None), check_vma=False
    )
```
